32 devices in a mesh: site: 2 (over core), replica: 4 (over z), model: 4 (over y, x).
Axes of the slice: x: 2, y: 2, z: 4, core: 2. Of those that a mesh axis runs over, the one named last changes fastest.
Arguments:
- partial_query: bfloat16 [8, 1024, 1024], P(('site', 'replica'), None, 'model'), parts along dimension 0, may hold values from -4 to 4
- partial_key: bfloat16 [8, 1024, 1024], P(('site', 'replica'), None, 'model'), parts along dimension 0, may hold values from -4 to 4
- partial_value: bfloat16 [8, 1024, 1024], P(('site', 'replica'), None, 'model'), parts along dimension 0, may hold values from -4 to 4
- partial_mixed: bfloat16 [8, 1024, 1024], P(('site', 'replica'), 'model'), parts along dimension 0, may hold values from -4 to 4
- partial_norm: bfloat16 [8, 1024], P(('site', 'replica')), parts along dimension 0, may hold values from -8 to 8
- master_query: float32 [2048, 1024], P(('site', 'replica'), 'model'), parts along dimension 0, may hold values from -0.1875 to 0.1875
- master_key: float32 [2048, 1024], P(('site', 'replica'), 'model'), parts along dimension 0, may hold values from -0.1875 to 0.1875
- master_value: float32 [2048, 1024], P(('site', 'replica'), 'model'), parts along dimension 0, may hold values from -0.1875 to 0.1875
- master_mixed: float32 [2048, 1024], P(('site', 'model'), 'replica'), parts along dimension 0, may hold values from -0.1875 to 0.1875
- master_norm: float32 [2048], P(('site', 'replica')), parts along dimension 0, may hold values from 0.25 to 1.75
- memory_query: float32 [2048, 1024], P(('site', 'replica'), 'model'), parts along dimension 0, may hold values from 0.05 to 0.8
- memory_key: float32 [2048, 1024], P(('site', 'replica'), 'model'), parts along dimension 0, may hold values from 0.05 to 0.8
- memory_value: float32 [2048, 1024], P(('site', 'replica'), 'model'), parts along dimension 0, may hold values from 0.05 to 0.8
- memory_mixed: float32 [2048, 1024], P(('site', 'model'), 'replica'), parts along dimension 0, may hold values from 0.05 to 0.8
- memory_norm: float32 [2048], P(('site', 'replica')), parts along dimension 0, may hold values from 0.05 to 0.8
Outputs:
- compute_query: bfloat16 [2048, 1024], P('site', 'model'), parts along dimension 0
- compute_key: bfloat16 [2048, 1024], P('site', 'model'), parts along dimension 0
- compute_value: bfloat16 [2048, 1024], P('site', 'model'), parts along dimension 0
- compute_mixed: bfloat16 [2048, 1024], P(('site', 'model')), parts along dimension 0
- compute_norm: bfloat16 [2048], P('site'), parts along dimension 0
- stepped_query: float32 [2048, 1024], P(('site', 'replica'), 'model'), parts along dimension 0
- stepped_key: float32 [2048, 1024], P(('site', 'replica'), 'model'), parts along dimension 0
- stepped_value: float32 [2048, 1024], P(('site', 'replica'), 'model'), parts along dimension 0
- stepped_mixed: float32 [2048, 1024], P(('site', 'model'), 'replica'), parts along dimension 0
- stepped_norm: float32 [2048], P(('site', 'replica')), parts along dimension 0
- state_new_query: float32 [2048, 1024], P(('site', 'replica'), 'model'), parts along dimension 0
- state_new_key: float32 [2048, 1024], P(('site', 'replica'), 'model'), parts along dimension 0
- state_new_value: float32 [2048, 1024], P(('site', 'replica'), 'model'), parts along dimension 0
- state_new_mixed: float32 [2048, 1024], P(('site', 'model'), 'replica'), parts along dimension 0
- state_new_norm: float32 [2048], P(('site', 'replica')), parts along dimension 0
The draws below stay inside these ranges and needn't reach their ends.
There are 2 independent parts, one for each index of `site`. The reference program is written for one: setup_inputs(seed, part) draws one part's arguments, and reference() takes and returns one part's arrays. A program takes and returns all parts, laid end to end along the dimension named above; each array names one. Nothing has to cross between parts.
All inputs are finite; a program needn't handle non-finite values.
Results may differ from the reference program's by a relative error of at most 0.001.
Values may be sent and summed in bfloat16 or wider, within the bound.
No kernel may reach another device: no remote copies, remote signals or barrier semaphores. Data moves between devices by JAX's collectives and lax.ppermute only.
A program may use at most 64 MiB of HBM per device.

```python
import jax
import jax.numpy as jnp
from jax import lax

WIDTH = 1024
ATTN = 1024
REPLICAS = 4


def spiked(values, rng, source, target, blocks, factor):
    def block_of(axis_at):
        return (jnp.arange(values.shape[axis_at]) // (values.shape[axis_at] // blocks)).reshape((-1,) + (1,) * (values.ndim - 1 - axis_at))

    one_side = jax.random.permutation(rng, blocks)[block_of(target)]
    second = (block_of(target) + blocks // 2) % blocks
    return jnp.where((block_of(source) == one_side) | (block_of(source) == second), factor * values, values)


def level_of(key, dims, cuts, least, largest):
    def one(dim, blocks):
        steps = jax.random.uniform(jax.random.fold_in(jax.random.fold_in(key, 6), dim), (blocks,), jnp.float32, least / len(cuts), largest / len(cuts))
        return jnp.repeat(jnp.exp(steps), dims[dim] // blocks).reshape((-1,) + (1,) * (len(dims) - dim - 1))

    gain = one(*cuts[0])
    for cut in cuts[1:]:
        gain = gain * one(*cut)
    return gain


def centred(own_key, dims, spread, bound, pieces=(), kind=jnp.bfloat16):
    drawn = spread * jax.random.normal(own_key, dims, jnp.float32)
    if pieces:
        drawn = drawn * level_of(own_key, dims, pieces, -0.22, 0.18)
    return jnp.clip(drawn, -bound, bound).astype(kind)


def bell_draw_with(stream_key, extent, spread, reach, shards, heavy, dtype=jnp.bfloat16):
    entries = spread * jax.random.normal(stream_key, extent, jnp.float32)
    if shards:
        entries = entries * level_of(stream_key, extent, shards, -0.22, 0.18)
    return jnp.clip(spiked(entries, jax.random.fold_in(stream_key, 3), *heavy), -reach, reach).astype(dtype)


def setup_inputs(seed: int = 0, part: int = 0) -> dict:
    splits = jax.random.split(jax.random.key(seed), 16)
    own_keys = jax.random.split(jax.random.fold_in(splits[15], part), 16)
    partial_query = bell_draw_with(own_keys[0], (REPLICAS, WIDTH, ATTN), 0.5, 4.0, ((0, 4), (2, 4)), (0, 1, 4, 2.0))
    partial_key = bell_draw_with(own_keys[1], (REPLICAS, WIDTH, ATTN), 0.5, 4.0, ((0, 4), (2, 4)), (0, 1, 4, 2.0))
    partial_value = bell_draw_with(own_keys[2], (REPLICAS, WIDTH, ATTN), 0.5, 4.0, ((0, 4), (2, 4)), (0, 1, 4, 2.0))
    partial_mixed = bell_draw_with(own_keys[3], (REPLICAS, ATTN, WIDTH), 0.5, 4.0, ((0, 4), (1, 4)), (0, 2, 4, 2.0))
    partial_norm = bell_draw_with(own_keys[4], (REPLICAS, WIDTH), 1.0, 8.0, ((0, 4),), (0, 1, 4, 2.0))
    master_query = centred(own_keys[5], (WIDTH, ATTN), WIDTH ** -0.5, 0.1875, ((0, 4), (1, 4)), jnp.float32)
    master_key = centred(own_keys[6], (WIDTH, ATTN), WIDTH ** -0.5, 0.1875, ((0, 4), (1, 4)), jnp.float32)
    master_value = centred(own_keys[7], (WIDTH, ATTN), WIDTH ** -0.5, 0.1875, ((0, 4), (1, 4)), jnp.float32)
    master_mixed = centred(own_keys[8], (ATTN, WIDTH), ATTN ** -0.5, 0.1875, ((0, 4), (1, 4)), jnp.float32)
    master_norm = jnp.clip(1.0 + 0.15 * jax.random.normal(own_keys[9], (WIDTH,), jnp.float32), 0.25, 1.75)
    memory_query = jnp.clip(0.05 + 0.75 * jax.random.uniform(own_keys[10], (WIDTH, ATTN), jnp.float32) ** level_of(own_keys[10], (WIDTH, ATTN), ((0, 4), (1, 4)), -0.2, 0.2), 0.05, 0.8)
    memory_key = jnp.clip(0.05 + 0.75 * jax.random.uniform(own_keys[11], (WIDTH, ATTN), jnp.float32) ** level_of(own_keys[11], (WIDTH, ATTN), ((0, 4), (1, 4)), -0.2, 0.2), 0.05, 0.8)
    memory_value = jnp.clip(0.05 + 0.75 * jax.random.uniform(own_keys[12], (WIDTH, ATTN), jnp.float32) ** level_of(own_keys[12], (WIDTH, ATTN), ((0, 4), (1, 4)), -0.2, 0.2), 0.05, 0.8)
    memory_mixed = jnp.clip(0.05 + 0.75 * jax.random.uniform(own_keys[13], (ATTN, WIDTH), jnp.float32) ** level_of(own_keys[13], (ATTN, WIDTH), ((0, 4), (1, 4)), -0.2, 0.2), 0.05, 0.8)
    memory_norm = jnp.clip(0.05 + 0.75 * jax.random.uniform(own_keys[14], (WIDTH,), jnp.float32) ** level_of(own_keys[14], (WIDTH,), ((0, 4),), -0.2, 0.2), 0.05, 0.8)
    return {"partial_query": partial_query, "partial_key": partial_key, "partial_value": partial_value, "partial_mixed": partial_mixed, "partial_norm": partial_norm, "master_query": master_query, "master_key": master_key, "master_value": master_value, "master_mixed": master_mixed, "master_norm": master_norm, "memory_query": memory_query, "memory_key": memory_key, "memory_value": memory_value, "memory_mixed": memory_mixed, "memory_norm": memory_norm}


learn_rate = 0.05
hold_rate = 0.7

def reference(partial_query, partial_key, partial_value, partial_mixed, partial_norm, master_query, master_key, master_value, master_mixed, master_norm, memory_query, memory_key, memory_value, memory_mixed, memory_norm):
    mean_query = lax.optimization_barrier(jnp.sum(partial_query.astype(jnp.float32), axis=0)) * REPLICAS ** (-0.5)
    mean_key = lax.optimization_barrier(jnp.sum(partial_key.astype(jnp.float32), axis=0)) * REPLICAS ** (-0.5)
    mean_value = lax.optimization_barrier(jnp.sum(partial_value.astype(jnp.float32), axis=0)) * REPLICAS ** (-0.5)
    mean_mixed = lax.optimization_barrier(jnp.sum(partial_mixed.astype(jnp.float32), axis=0)) * REPLICAS ** (-0.5)
    mean_norm = lax.optimization_barrier(jnp.sum(partial_norm.astype(jnp.float32), axis=0)) * REPLICAS ** (-0.5)
    state_new_query = hold_rate * memory_query + (1.0 - hold_rate) * mean_query * mean_query
    stepped_query = master_query - learn_rate * mean_query * lax.rsqrt(state_new_query + 1e-06)
    state_new_key = hold_rate * memory_key + (1.0 - hold_rate) * mean_key * mean_key
    stepped_key = master_key - learn_rate * mean_key * lax.rsqrt(state_new_key + 1e-06)
    state_new_value = hold_rate * memory_value + (1.0 - hold_rate) * mean_value * mean_value
    stepped_value = master_value - learn_rate * mean_value * lax.rsqrt(state_new_value + 1e-06)
    state_new_mixed = hold_rate * memory_mixed + (1.0 - hold_rate) * mean_mixed * mean_mixed
    stepped_mixed = master_mixed - learn_rate * mean_mixed * lax.rsqrt(state_new_mixed + 1e-06)
    state_new_norm = hold_rate * memory_norm + (1.0 - hold_rate) * mean_norm * mean_norm
    stepped_norm = master_norm - learn_rate * mean_norm * lax.rsqrt(state_new_norm + 1e-06)
    compute_query = stepped_query.astype(jnp.bfloat16)
    compute_key = stepped_key.astype(jnp.bfloat16)
    compute_value = stepped_value.astype(jnp.bfloat16)
    compute_mixed = stepped_mixed.astype(jnp.bfloat16)
    compute_norm = stepped_norm.astype(jnp.bfloat16)
    return (compute_query, compute_key, compute_value, compute_mixed, compute_norm, stepped_query, stepped_key, stepped_value, stepped_mixed, stepped_norm, state_new_query, state_new_key, state_new_value, state_new_mixed, state_new_norm)
```

```python
import jax
import jax.numpy as jnp
from jax import lax
from jax.sharding import PartitionSpec as P

learn_rate = 0.05
hold_rate = 0.7
GROUPS = ((0, 1), (2, 3))


def cut(x, place, parts, axis):
    size = x.shape[axis] // parts
    return lax.dynamic_slice_in_dim(x, place * size, size, axis)


def update(mean, master, memory):
    state = hold_rate * memory + (1.0 - hold_rate) * mean * mean
    return master - learn_rate * mean * lax.rsqrt(state + 1e-06), state


def shift(x, step, parts):
    return lax.ppermute(x, "replica", [(k, (k + step) % parts) for k in range(parts)])


def place_pieces(pieces, me, axis):
    parts = len(pieces)
    size = pieces[0].shape[axis]
    shape = list(pieces[0].shape)
    shape[axis] = size * parts
    out = jnp.zeros(shape, pieces[0].dtype)
    for step, piece in enumerate(pieces):
        out = lax.dynamic_update_slice_in_dim(out, piece, (me + parts - step) % parts * size, axis)
    return out


def gather(mine, axis_list, me, parts):
    packed = jnp.concatenate(mine, axis=0)
    up, down = packed, packed
    got = {0: packed}
    for s in range(1, parts // 2 + 1):
        up = shift(up, 1, parts)
        got[s] = up
        if parts - s not in got:
            down = shift(down, parts - 1, parts)
            got[parts - s] = down
    pieces = [got[s] for s in range(parts)]
    outs, row = [], 0
    for m, a in zip(mine, axis_list):
        h = m.shape[0]
        outs.append(place_pieces([p[row:row + h] for p in pieces], me, a))
        row += h
    return outs


def few(*args):
    partials, masters, memories = args[:5], args[5:10], args[10:]
    parts = lax.axis_size("replica")
    me = lax.axis_index("replica")
    rate = parts ** (-0.5)
    axes = (0, 0, 0, 1)
    compute, stepped, state = [None] * 5, [None] * 5, [None] * 5
    pn = partials[4][0].reshape(parts, -1)
    norm_in = [lax.dynamic_index_in_dim(pn, (me + s) % parts, 0, keepdims=True) for s in range(parts)]
    norm_in = [norm_in[0]] + [shift(norm_in[s], s, parts) for s in range(1, parts)]
    mean_norm = sum(x[0].astype(jnp.float32) for x in norm_in) * rate
    stepped[4], state[4] = update(mean_norm, masters[4], memories[4])
    low = stepped[4].astype(jnp.bfloat16)[None]
    npieces = [low] + [shift(low, s, parts) for s in range(1, parts)]
    compute[4] = place_pieces(npieces, me, 0).reshape(-1)
    for group in GROUPS:
        got = [[cut(partials[t][0], me, parts, axes[t]).astype(jnp.float32) for t in group]]
        for s in range(1, parts):
            packed = jnp.concatenate([cut(partials[t][0], (me + s) % parts, parts, axes[t]) for t in group], axis=0)
            packed = shift(packed, s, parts)
            h = packed.shape[0] // len(group)
            got.append([packed[k * h:(k + 1) * h].astype(jnp.float32) for k in range(len(group))])
        sums = [sum(g[k] for g in got) for k in range(len(group))]
        lows = []
        for t, total in zip(group, sums):
            stepped[t], state[t] = update(total * rate, masters[t], memories[t])
            lows.append(stepped[t].astype(jnp.bfloat16))
        for t, o in zip(group, gather(lows, [axes[t] for t in group], me, parts)):
            compute[t] = o
    return tuple(compute + stepped + state)


def plain(
    partial_query,
    partial_key,
    partial_value,
    partial_mixed,
    partial_norm,
    master_query,
    master_key,
    master_value,
    master_mixed,
    master_norm,
    memory_query,
    memory_key,
    memory_value,
    memory_mixed,
    memory_norm,
):
    mean_query, mean_key, mean_value, mean_mixed = (
        lax.psum_scatter(
            partial_query[0].astype(jnp.float32), "replica", scatter_dimension=0, tiled=True
        ),
        lax.psum_scatter(
            partial_key[0].astype(jnp.float32), "replica", scatter_dimension=0, tiled=True
        ),
        lax.psum_scatter(
            partial_value[0].astype(jnp.float32), "replica", scatter_dimension=0, tiled=True
        ),
        lax.psum_scatter(
            partial_mixed[0].astype(jnp.float32), "replica", scatter_dimension=1, tiled=True
        ),
    )
    whole_norm = lax.psum(partial_norm[0].astype(jnp.float32), "replica")
    place = lax.axis_index("replica")
    mean_norm = lax.dynamic_slice_in_dim(
        whole_norm, place * master_norm.shape[0], master_norm.shape[0]
    )
    mean_rate = lax.axis_size("replica") ** (-0.5)
    mean_query = mean_query * mean_rate
    mean_key = mean_key * mean_rate
    mean_value = mean_value * mean_rate
    mean_mixed = mean_mixed * mean_rate
    mean_norm = mean_norm * mean_rate
    state_new_query = hold_rate * memory_query + (1.0 - hold_rate) * mean_query * mean_query
    stepped_query = master_query - learn_rate * mean_query * lax.rsqrt(state_new_query + 1e-06)
    state_new_key = hold_rate * memory_key + (1.0 - hold_rate) * mean_key * mean_key
    stepped_key = master_key - learn_rate * mean_key * lax.rsqrt(state_new_key + 1e-06)
    state_new_value = hold_rate * memory_value + (1.0 - hold_rate) * mean_value * mean_value
    stepped_value = master_value - learn_rate * mean_value * lax.rsqrt(state_new_value + 1e-06)
    state_new_mixed = hold_rate * memory_mixed + (1.0 - hold_rate) * mean_mixed * mean_mixed
    stepped_mixed = master_mixed - learn_rate * mean_mixed * lax.rsqrt(state_new_mixed + 1e-06)
    state_new_norm = hold_rate * memory_norm + (1.0 - hold_rate) * mean_norm * mean_norm
    stepped_norm = master_norm - learn_rate * mean_norm * lax.rsqrt(state_new_norm + 1e-06)
    compute_query, compute_key, compute_value, compute_mixed, compute_norm = (
        lax.all_gather(stepped_query.astype(jnp.bfloat16), "replica", axis=0, tiled=True),
        lax.all_gather(stepped_key.astype(jnp.bfloat16), "replica", axis=0, tiled=True),
        lax.all_gather(stepped_value.astype(jnp.bfloat16), "replica", axis=0, tiled=True),
        lax.all_gather(stepped_mixed.astype(jnp.bfloat16), "replica", axis=1, tiled=True),
        lax.all_gather(stepped_norm.astype(jnp.bfloat16), "replica", axis=0, tiled=True),
    )
    return (
        compute_query,
        compute_key,
        compute_value,
        compute_mixed,
        compute_norm,
        stepped_query,
        stepped_key,
        stepped_value,
        stepped_mixed,
        stepped_norm,
        state_new_query,
        state_new_key,
        state_new_value,
        state_new_mixed,
        state_new_norm,
    )


def body(*args):
    parts = lax.axis_size("replica")
    tall = (args[0].shape[1] // parts, args[0].shape[2])
    wide = (args[3].shape[1], args[3].shape[2] // parts)
    if parts <= 4 and tall == wide:
        return few(*args)
    return plain(*args)


def solution(mesh):
    placed = (
        P(("site", "replica"), None, "model"),
        P(("site", "replica"), None, "model"),
        P(("site", "replica"), None, "model"),
        P(("site", "replica"), "model", None),
        P(("site", "replica"), None),
        P(("site", "replica"), "model"),
        P(("site", "replica"), "model"),
        P(("site", "replica"), "model"),
        P(("site", "model"), "replica"),
        P(("site", "replica")),
        P(("site", "replica"), "model"),
        P(("site", "replica"), "model"),
        P(("site", "replica"), "model"),
        P(("site", "model"), "replica"),
        P(("site", "replica")),
    )
    return jax.shard_map(
        body,
        mesh=mesh,
        in_specs=placed,
        out_specs=(
            P("site", "model"),
            P("site", "model"),
            P("site", "model"),
            P(("site", "model"), None),
            P("site"),
            P(("site", "replica"), "model"),
            P(("site", "replica"), "model"),
            P(("site", "replica"), "model"),
            P(("site", "model"), "replica"),
            P(("site", "replica")),
            P(("site", "replica"), "model"),
            P(("site", "replica"), "model"),
            P(("site", "replica"), "model"),
            P(("site", "model"), "replica"),
            P(("site", "replica")),
        ),
        check_vma=False,
    )
```
